512 devices in a mesh: group: 2 (over y), ctx: 8 (over x), ep: 32 (over z, core).
Axes of the slice: x: 8, y: 2, z: 16, core: 2. Of those that a mesh axis runs over, the one named last changes fastest.
The devices are a block of a 8x8x16 slice.
Arguments:
- q_latent: bfloat16 [2048, 65536], P(('group', 'ctx'), 'ep'), parts along dimension 0, may hold values from -48 to 48
- q_rope: bfloat16 [2048, 8192], P(('group', 'ctx'), 'ep'), parts along dimension 0, may hold values from -6 to 6
- latent_keys: bfloat16 [1024, 1024], P('group', 'ctx'), parts along dimension 0, may hold values from -8 to 8
- rope_keys: bfloat16 [128, 1024], P('group', 'ctx'), parts along dimension 0, may hold values from -8 to 8
- w_uv: bfloat16 [128, 512, 128], P('ep'), may hold values from -0.25 to 0.25
- moe_tokens: bfloat16 [16384, 7168], P(('group', 'ep'), 'ctx'), parts along dimension 0, may hold values from -6 to 6
- norm_gain: float32 [7168], P('ctx'), may hold values from 0.1 to 1.9
- expert_ids: int32 [16384, 2], P(('group', 'ep')), parts along dimension 0, may hold values from 0 to 15, all different within a row; in each aligned block of 256 rows (0 to 255, 256 to 511, ...) at most 48 rows name the same one
- route_scale: float32 [16384, 2], P(('group', 'ep')), parts along dimension 0, may hold values from 0.5 to 2.5
- w_gate: bfloat16 [32, 7168, 512], P('ep', 'ctx'), may hold values from -0.0625 to 0.0625
- w_up: bfloat16 [32, 7168, 512], P('ep', 'ctx'), may hold values from -0.0625 to 0.0625
- w_down: bfloat16 [32, 512, 7168], P('ep', None, 'ctx'), may hold values from -0.1875 to 0.1875
Outputs:
- attn_out: bfloat16 [2048, 16384], P(('group', 'ctx'), 'ep'), parts along dimension 0
- moe_out: bfloat16 [16384, 7168], P(('group', 'ep'), 'ctx'), parts along dimension 0
The draws below stay inside these ranges and needn't reach their ends.
There are 2 independent parts, one for each index of `group`. The reference program is written for one: setup_inputs(seed, part) draws one part's arguments, and reference() takes and returns one part's arrays. A program takes and returns all parts, laid end to end along the dimension named above; an argument that names none is the same for every part. Nothing has to cross between parts.
Inputs may be any that keep to these rules, and one draw needn't show every extreme that they name: `expert_ids`: each row names 2 different experts; among the rows of one ep index no expert is named more than 48 times, a bound that some block reaches.
All inputs are finite; a program needn't handle non-finite values.
Results may differ from the reference program's by a relative error of at most 0.024.
Values may be sent and summed in bfloat16 or wider, within the bound.
No kernel may reach another device: no remote copies, remote signals or barrier semaphores. Data moves between devices by JAX's collectives and lax.ppermute only.
A program may use at most 64 MiB of HBM per device.

```python
import math
import jax
import jax.numpy as jnp
import numpy as np
from jax import lax

D = 7168
LATENT = 512
ROPE = 64
VDIM = 128
FF = 1024
TOP = 2
TOK_DEV = 256
SEQ = 1024
HEADS = 128
MTOK = 8192
EXP = 16
FH = 512
CAP = 48
N_EP = 32


def attention_draw(base_key):
    key_base = jax.random.fold_in(base_key, 41)
    keys_all = jax.random.split(key_base, 4)
    query_lat = jnp.clip(jax.random.normal(keys_all[0], (SEQ, HEADS, LATENT), jnp.float32), -6.0, 6.0)
    query_rot = jnp.clip(jax.random.normal(keys_all[1], (SEQ, HEADS, ROPE), jnp.float32), -6.0, 6.0)
    key_lat = jnp.clip(jax.random.normal(keys_all[2], (SEQ, LATENT), jnp.float32), -6.0, 6.0)
    key_rot = jnp.clip(jax.random.normal(keys_all[3], (SEQ, ROPE), jnp.float32), -6.0, 6.0)
    return (query_lat.reshape(SEQ, HEADS * LATENT), query_rot.reshape(SEQ, HEADS * ROPE), key_lat.T, key_rot.T)


def draw_q_latent(key, part):
    return attention_draw(key)[0].astype(jnp.bfloat16)


def draw_q_rope(key, part):
    return attention_draw(key)[1].astype(jnp.bfloat16)


def draw_latent_keys(key, part):
    return attention_draw(key)[2].astype(jnp.bfloat16)


def draw_rope_keys(key, part):
    return attention_draw(key)[3].astype(jnp.bfloat16)


def shard_levels(rng, shape, cuts, least, high):
    loudness, own = 1.0, jax.random.fold_in(rng, 6)
    for axis_at, parts in cuts:
        steps = jnp.exp(jax.random.uniform(jax.random.fold_in(own, axis_at), (parts,), jnp.float32, least / len(cuts), high / len(cuts)))
        loudness = loudness * jnp.repeat(steps, shape[axis_at] // parts).reshape([-1 if axis == axis_at else 1 for axis in range(len(shape))])
    return loudness


def deal_out(rng, own, number, rows, amount, top, bound, skew):
    sequence = jax.random.permutation(rng, amount)
    packed, usual = load_shares(amount, rows * top, bound, skew, True), load_shares(amount, rows * top, bound, skew, False)
    places = jnp.arange(amount)

    def named(tallies, turn):
        used = int((tallies > 0).sum())
        fixed = max(1, used // 4)
        moved = fixed + (places - fixed + turn * (used - fixed)) % max(1, amount - fixed)
        return jnp.zeros((amount,), jnp.int32).at[sequence[jnp.where(places < fixed, places, moved)]].set(jnp.asarray(tallies, jnp.int32))

    tallies = jnp.where(number % 4 == 0, named(packed, number // 4), named(usual, number - number // 4 - 1))
    mixed = jax.random.permutation(jax.random.fold_in(own, 3), amount)
    giver, taker = mixed[0:amount // 2 * 2:2], mixed[1:amount // 2 * 2:2]
    slack = jnp.minimum(tallies[giver] - 1, bound - tallies[taker]) // 2
    slack = jnp.where((giver == sequence[0]) | (taker == sequence[0]) | (tallies[taker] == 0), 0, jnp.maximum(slack, 0))
    moved = jax.random.randint(jax.random.fold_in(own, 4), (amount // 2,), 0, 1 << 20) % (slack + 1)
    tallies = tallies.at[giver].add(-moved).at[taker].add(moved)
    members = jnp.searchsorted(jnp.cumsum(tallies), jnp.arange(rows * top), side="right").astype(jnp.int32)
    listing = members.reshape(top, rows).T
    listing = listing[jax.random.permutation(jax.random.fold_in(own, 1), rows)]
    turn = jax.random.randint(jax.random.fold_in(own, 2), (rows, 1), 0, top)
    return jnp.take_along_axis(listing, (jnp.arange(top)[None, :] + turn) % top, axis=1)


def load_shares(number_of, total, limit, lean, full):
    portions = [(1 << 20) // math.isqrt(standing ** lean) + 1 for standing in range(1, number_of + 1)]
    largest = limit if full else min(limit, max(-(-total // number_of), total * portions[0] // sum(portions)))
    least = 1 if total - largest >= number_of - 1 else 0
    given, rest = [largest] + [least] * (number_of - 1), total - largest - least * (number_of - 1)
    while rest > 0:
        movable = [i for i in range(1, number_of) if given[i] < largest] or [i for i in range(1, number_of) if given[i] < limit]
        pool, left = sum([portions[i] for i in movable]), rest
        for i in movable:
            extra = min(limit - given[i], max(1, left * portions[i] // pool), rest)
            given[i] = given[i] + extra
            rest = rest - extra
    return np.array(given)


def bell_draw(rng, shape, scale, most, pieces=(), kind=jnp.bfloat16):
    values = jax.random.normal(rng, shape, jnp.float32) * scale
    if len(pieces) > 0:
        values = shard_levels(rng, shape, pieces, -0.22, 0.18) * values
    return jnp.clip(values, min=-most, max=most).astype(kind)


def setup_inputs(seed: int = 0, part: int = 0) -> dict:
    seeds = jax.random.split(jax.random.key(seed), 13)
    own_keys = jax.random.split(jax.random.fold_in(seeds[12], part), 13)
    q_latent = draw_q_latent(jax.random.fold_in(jax.random.fold_in(seeds[12], part), 71), part)
    q_rope = draw_q_rope(jax.random.fold_in(jax.random.fold_in(seeds[12], part), 71), part)
    latent_keys = draw_latent_keys(jax.random.fold_in(jax.random.fold_in(seeds[12], part), 71), part)
    rope_keys = draw_rope_keys(jax.random.fold_in(jax.random.fold_in(seeds[12], part), 71), part)
    w_uv = bell_draw(seeds[4], (HEADS, LATENT, VDIM), LATENT ** -0.5, 0.25, ((0, 32),))
    moe_tokens = bell_draw(own_keys[5], (MTOK, D), 1.0, 6.0, ((0, 32), (1, 8)))
    norm_gain = jnp.clip(1.0 + 0.18 * jax.random.normal(seeds[6], (D,), jnp.float32), 0.1, 1.9)
    expert_ids_keys = jax.random.split(jax.random.fold_in(own_keys[7], 1), MTOK // TOK_DEV)
    expert_ids_turns = jax.random.permutation(jax.random.fold_in(own_keys[7], 3), MTOK // TOK_DEV)
    expert_ids = jax.vmap(lambda own, number: deal_out(jax.random.fold_in(own_keys[7], 2), own, number, TOK_DEV, EXP, TOP, CAP, 2))(expert_ids_keys, expert_ids_turns).reshape((MTOK, TOP))
    route_scale = jnp.clip(0.5 + 2.0 * jax.random.uniform(own_keys[8], (MTOK, TOP), jnp.float32) ** shard_levels(own_keys[8], (MTOK, TOP), ((0, 32),), -0.2, 0.2), 0.5, 2.5)
    w_gate = bell_draw(seeds[9], (2 * EXP, D, FH), D ** -0.5, 0.0625, ((0, 32), (1, 8)))
    w_up = bell_draw(seeds[10], (2 * EXP, D, FH), D ** -0.5, 0.0625, ((0, 32), (1, 8)))
    w_down = bell_draw(seeds[11], (2 * EXP, FH, D), FF ** -0.5, 0.1875, ((0, 32), (2, 8)))
    return dict(q_latent=q_latent, q_rope=q_rope, latent_keys=latent_keys, rope_keys=rope_keys, w_uv=w_uv, moe_tokens=moe_tokens, norm_gain=norm_gain, expert_ids=expert_ids, route_scale=route_scale, w_gate=w_gate, w_up=w_up, w_down=w_down)


score_scale = 192.0 ** (-0.5)
norm_eps = 1e-06

def reference(q_latent, q_rope, latent_keys, rope_keys, w_uv, moe_tokens, norm_gain, expert_ids, route_scale, w_gate, w_up, w_down):
    positions = jnp.arange(SEQ, dtype=jnp.int32)
    visible = positions[None, :] <= positions[:, None]

    def one_head(head_index):
        query_lat = lax.dynamic_slice_in_dim(q_latent, head_index * LATENT, LATENT, 1)
        query_rot = lax.dynamic_slice_in_dim(q_rope, head_index * ROPE, ROPE, 1)
        scores = jnp.dot(query_lat, latent_keys, preferred_element_type=jnp.float32)
        scores = (scores + jnp.dot(query_rot, rope_keys, preferred_element_type=jnp.float32)) * score_scale
        scores = jnp.where(visible, scores, -jnp.inf)
        row_max = lax.optimization_barrier(jnp.max(scores, axis=1, keepdims=True))
        exponent = jnp.exp(scores - row_max)
        row_total = lax.optimization_barrier(jnp.sum(exponent, axis=1, keepdims=True))
        probabilities = exponent.astype(jnp.bfloat16)
        mixed = jnp.dot(probabilities, latent_keys.T, preferred_element_type=jnp.float32) / row_total
        context = mixed.astype(jnp.bfloat16)
        return jnp.dot(context, w_uv[head_index], preferred_element_type=jnp.float32).astype(jnp.bfloat16)
    heads_out = lax.map(one_head, jnp.arange(HEADS, dtype=jnp.int32))
    attn_out = heads_out.transpose(1, 0, 2).reshape(SEQ, HEADS * VDIM)
    tokens_wide = moe_tokens.astype(jnp.float32)
    mean_square = lax.optimization_barrier(jnp.mean(tokens_wide * tokens_wide, axis=1, keepdims=True))
    normed = (tokens_wide * lax.rsqrt(mean_square + norm_eps) * norm_gain[None, :]).astype(jnp.bfloat16)
    flat_ids = expert_ids.reshape(-1)
    route_token = jnp.arange(MTOK * TOP, dtype=jnp.int32) // TOP
    source = route_token // TOK_DEV
    onehot = (flat_ids[:, None] == jnp.arange(EXP, dtype=jnp.int32)[None, :]).astype(jnp.int32)
    blocked = onehot.reshape(N_EP, TOK_DEV * TOP, EXP)
    slot_index = lax.optimization_barrier(jnp.sum((jnp.cumsum(blocked, axis=1) - blocked) * blocked, axis=2)).reshape(-1)
    row_index = source * CAP + slot_index
    scale_flat = route_scale.reshape(-1)
    total_rows = N_EP * CAP

    def scan_step(running, expert_index):
        chosen = flat_ids == expert_index
        destination = jnp.where(chosen, row_index, total_rows).astype(jnp.int32)
        token_at = jnp.zeros((total_rows,), jnp.int32).at[destination].set(route_token, mode='drop')
        scale_at = jnp.zeros((total_rows,), jnp.float32).at[destination].set(scale_flat, mode='drop')
        rows_taken = normed[token_at]
        output_sum = jnp.zeros((total_rows, D), jnp.float32)
        for half_index in range(2):
            block_index = 2 * expert_index + half_index
            gate_val = jnp.dot(rows_taken, w_gate[block_index], preferred_element_type=jnp.float32)
            up_val = jnp.dot(rows_taken, w_up[block_index], preferred_element_type=jnp.float32)
            hidden = (jax.nn.silu(gate_val) * up_val).astype(jnp.bfloat16)
            piece_out = jnp.dot(hidden, w_down[block_index], preferred_element_type=jnp.float32).astype(jnp.bfloat16)
            piece_out = lax.optimization_barrier(piece_out)
            output_sum = output_sum + piece_out.astype(jnp.float32)
        contribution = output_sum * scale_at[:, None]
        return (running + jax.ops.segment_sum(contribution, token_at, num_segments=MTOK), None)
    moe_sum, ignored = lax.scan(scan_step, jnp.zeros((MTOK, D), jnp.float32), jnp.arange(EXP, dtype=jnp.int32))
    return (attn_out, moe_sum.astype(jnp.bfloat16))
```

```python
import jax
import jax.numpy as jnp
from jax import lax
from jax.sharding import PartitionSpec as P

score_scale = 192.0 ** (-0.5)
norm_eps = 1e-06
neg_large = -1e30
lanes = 128


def in_one_piece(arrays, axis, dim, along):
    ends, at = ([], 0)
    for a in arrays[:-1]:
        at += a.shape[along]
        ends.append(at)
    both = jnp.concatenate(arrays, axis=along)
    return tuple(jnp.split(lax.all_gather(both, axis, axis=dim, tiled=True), ends, axis=along))


def same_core(axis):
    count = lax.axis_size(axis)
    return [list(range(core, count, 2)) for core in range(2)]


def of_other_core(value, axis):
    count = lax.axis_size(axis)
    return lax.ppermute(value, axis, [(i, i ^ 1) for i in range(count)])


def attention(q_latent, q_rope, lat_piece, rope_piece, w_uv):
    seq_rows = q_latent.shape[0]
    head_count, latent_dim = w_uv.shape[:2]
    rope_dim = rope_piece.shape[0]
    query_lat = (
        q_latent.reshape(seq_rows, head_count, latent_dim)
        .transpose(1, 0, 2)
        .reshape(head_count * seq_rows, latent_dim)
    )
    query_rot = (
        q_rope.reshape(seq_rows, head_count, rope_dim)
        .transpose(1, 0, 2)
        .reshape(head_count * seq_rows, rope_dim)
    )
    query_pos = lax.axis_index("ctx") * seq_rows + jnp.tile(
        jnp.arange(seq_rows, dtype=jnp.int32), head_count
    )
    scores = jnp.dot(query_lat, lat_piece, preferred_element_type=jnp.float32)
    scores = (
        scores + jnp.dot(query_rot, rope_piece, preferred_element_type=jnp.float32)
    ) * score_scale
    key_pos = jnp.arange(lat_piece.shape[1], dtype=jnp.int32)
    visible = key_pos[None, :] <= query_pos[:, None]
    masked = jnp.where(visible, scores, neg_large)
    row_max = jnp.max(masked, axis=1, keepdims=True)
    weights = jnp.where(visible, jnp.exp(masked - row_max), 0.0)
    row_sum = jnp.sum(weights, axis=1, keepdims=True)
    update = lax.dot_general(
        weights.astype(jnp.bfloat16),
        lat_piece,
        (((1,), (1,)), ((), ())),
        preferred_element_type=jnp.float32,
    )
    context = (update / row_sum).astype(jnp.bfloat16).reshape(head_count, seq_rows, latent_dim)
    attn_heads = jnp.einsum("hsl,hlv->shv", context, w_uv, preferred_element_type=jnp.float32)
    return attn_heads.reshape(seq_rows, head_count * w_uv.shape[2]).astype(jnp.bfloat16)


def body(
    q_latent,
    q_rope,
    latent_keys,
    rope_keys,
    w_uv,
    moe_tokens,
    norm_gain,
    expert_ids,
    route_scale,
    w_gate,
    w_up,
    w_down,
):
    lat_piece, rope_piece = in_one_piece((latent_keys, rope_keys), "ctx", 1, 0)
    model_width = moe_tokens.shape[1] * lax.axis_size("ctx")
    half_width = w_gate.shape[2]
    own_in = jnp.concatenate([w_gate[0], w_up[0]], axis=1)
    in_w = jnp.concatenate([own_in, of_other_core(own_in, "ep")], axis=1)
    down_w = jnp.concatenate([w_down[0], of_other_core(w_down[0], "ep")], axis=0)

    tok_rows, top_count = expert_ids.shape
    expert_count = lax.axis_size("ep") // 2
    capacity = min(tok_rows, 3 * tok_rows * top_count // (2 * expert_count))
    flat_ids = expert_ids.reshape(-1)
    onehot = (flat_ids[:, None] == jnp.arange(expert_count, dtype=jnp.int32)[None, :]).astype(
        jnp.int32
    )
    slot_index = jnp.sum((jnp.cumsum(onehot, axis=0) - onehot) * onehot, axis=1)
    target_slot = flat_ids * capacity + slot_index
    place_map = (
        target_slot[:, None] == jnp.arange(expert_count * capacity, dtype=jnp.int32)[None, :]
    ).astype(jnp.float32)
    place_map = place_map.reshape(tok_rows, top_count, expert_count * capacity)
    route_map = jnp.sum(place_map, axis=1)
    weight_map = jnp.sum(place_map * route_scale[:, :, None], axis=1)
    send_rows = jnp.dot(
        route_map.T.astype(jnp.bfloat16), moe_tokens, preferred_element_type=jnp.float32
    ).astype(jnp.bfloat16)
    arrived = lax.all_to_all(
        send_rows.reshape(expert_count, capacity, -1),
        "ep",
        split_axis=0,
        concat_axis=0,
        tiled=True,
        axis_index_groups=same_core("ep"),
    )
    rows_in = arrived.reshape(-1, arrived.shape[2])
    rows_wide = rows_in.astype(jnp.float32)
    row_sq = jnp.sum(rows_wide * rows_wide, axis=1, keepdims=True)
    gained = (rows_wide * norm_gain[None, :]).astype(jnp.bfloat16)
    in_part = jnp.dot(gained, in_w, preferred_element_type=jnp.float32).astype(jnp.bfloat16)
    row_share = lax.psum_scatter(
        jnp.concatenate(
            [in_part, jnp.broadcast_to(row_sq, (row_sq.shape[0], lanes)).astype(jnp.bfloat16)], axis=1
        ),
        "ctx",
        scatter_dimension=0,
        tiled=True,
    ).astype(jnp.float32)
    row_scale = lax.rsqrt(row_share[:, -1:] / model_width + norm_eps)
    sums = row_share[:, :-lanes] * row_scale
    part_hidden = jnp.concatenate(
        [
            jax.nn.silu(sums[:, at : at + half_width]) * sums[:, at + half_width : at + 2 * half_width]
            for at in (0, 2 * half_width)
        ],
        axis=1,
    ).astype(jnp.bfloat16)
    hidden = lax.all_gather(part_hidden, "ctx", axis=0, tiled=True)
    expert_out = (
        jnp.dot(hidden, down_w, preferred_element_type=jnp.float32)
        .astype(jnp.bfloat16)
        .reshape(arrived.shape)
    )
    returned = lax.all_to_all(
        expert_out,
        "ep",
        split_axis=0,
        concat_axis=0,
        tiled=True,
        axis_index_groups=same_core("ep"),
    ).reshape(expert_count * capacity, -1)
    weight_high = weight_map.astype(jnp.bfloat16)
    weight_low = (weight_map - weight_high.astype(jnp.float32)).astype(jnp.bfloat16)
    moe_out = (
        jnp.dot(weight_high, returned, preferred_element_type=jnp.float32)
        + jnp.dot(weight_low, returned, preferred_element_type=jnp.float32)
    ).astype(jnp.bfloat16)
    attn_out = attention(q_latent, q_rope, lat_piece, rope_piece, w_uv)
    return (attn_out, moe_out)


def solution(mesh):
    return jax.shard_map(
        body,
        mesh=mesh,
        in_specs=(
            P(("group", "ctx"), "ep"),
            P(("group", "ctx"), "ep"),
            P("group", "ctx"),
            P("group", "ctx"),
            P("ep", None, None),
            P(("group", "ep"), "ctx"),
            P("ctx"),
            P(("group", "ep"), None),
            P(("group", "ep"), None),
            P("ep", "ctx", None),
            P("ep", "ctx", None),
            P("ep", None, "ctx"),
        ),
        out_specs=(P(("group", "ctx"), "ep"), P(("group", "ep"), "ctx")),
        check_vma=False,
    )
```

```python
import jax
import jax.numpy as jnp
from jax import lax
from jax.sharding import PartitionSpec as P

score_scale = 192.0 ** (-0.5)
norm_eps = 1e-06
neg_large = -1e30
lanes = 128


def in_one_piece(arrays, axis, dim, along):
    ends, at = ([], 0)
    for a in arrays[:-1]:
        at += a.shape[along]
        ends.append(at)
    both = jnp.concatenate(arrays, axis=along)
    return tuple(jnp.split(lax.all_gather(both, axis, axis=dim, tiled=True), ends, axis=along))


def same_core(axis):
    count = lax.axis_size(axis)
    return [list(range(core, count, 2)) for core in range(2)]


def of_other_core(value, axis):
    count = lax.axis_size(axis)
    return lax.ppermute(value, axis, [(i, i ^ 1) for i in range(count)])


def attention(q_latent, q_rope, lat_piece, rope_piece, w_uv):
    seq_rows = q_latent.shape[0]
    head_count, latent_dim = w_uv.shape[:2]
    rope_dim = rope_piece.shape[0]
    query_lat = (
        q_latent.reshape(seq_rows, head_count, latent_dim)
        .transpose(1, 0, 2)
        .reshape(head_count * seq_rows, latent_dim)
    )
    query_rot = (
        q_rope.reshape(seq_rows, head_count, rope_dim)
        .transpose(1, 0, 2)
        .reshape(head_count * seq_rows, rope_dim)
    )
    query_pos = lax.axis_index("ctx") * seq_rows + jnp.tile(
        jnp.arange(seq_rows, dtype=jnp.int32), head_count
    )
    scores = jnp.dot(query_lat, lat_piece, preferred_element_type=jnp.float32)
    scores = (
        scores + jnp.dot(query_rot, rope_piece, preferred_element_type=jnp.float32)
    ) * score_scale
    key_pos = jnp.arange(lat_piece.shape[1], dtype=jnp.int32)
    visible = key_pos[None, :] <= query_pos[:, None]
    masked = jnp.where(visible, scores, neg_large)
    row_max = jnp.max(masked, axis=1, keepdims=True)
    weights = jnp.where(visible, jnp.exp(masked - row_max), 0.0)
    row_sum = jnp.sum(weights, axis=1, keepdims=True)
    update = lax.dot_general(
        weights.astype(jnp.bfloat16),
        lat_piece,
        (((1,), (1,)), ((), ())),
        preferred_element_type=jnp.float32,
    )
    context = (update / row_sum).astype(jnp.bfloat16).reshape(head_count, seq_rows, latent_dim)
    attn_heads = jnp.einsum("hsl,hlv->shv", context, w_uv, preferred_element_type=jnp.float32)
    return attn_heads.reshape(seq_rows, head_count * w_uv.shape[2]).astype(jnp.bfloat16)


def sent_rows(route_map, tokens):
    return jnp.dot(route_map.T, tokens, preferred_element_type=jnp.float32).astype(jnp.bfloat16)


def to_same_core(rows, count):
    return lax.all_to_all(
        rows.reshape(count, -1, rows.shape[1]),
        "ep",
        split_axis=0,
        concat_axis=0,
        tiled=True,
        axis_index_groups=same_core("ep"),
    ).reshape(rows.shape)


def activation_sums(rows, norm_gain, in_w):
    rows_wide = rows.astype(jnp.float32)
    row_sq = jnp.sum(rows_wide * rows_wide, axis=1, keepdims=True)
    gained = (rows_wide * norm_gain[None, :]).astype(jnp.bfloat16)
    in_part = jnp.dot(gained, in_w, preferred_element_type=jnp.float32)
    column = lax.broadcasted_iota(jnp.int32, in_part.shape, 1)
    in_part = jnp.where(column < in_w.shape[1] - lanes, in_part, row_sq).astype(jnp.bfloat16)
    return lax.psum_scatter(in_part, "ctx", scatter_dimension=0, tiled=True)


def activations(row_share, model_width, half_width):
    row_share = row_share.astype(jnp.float32)
    row_scale = lax.rsqrt(row_share[:, -1:] / model_width + norm_eps)
    sums = row_share[:, :-lanes] * row_scale
    part_hidden = jnp.concatenate(
        [
            jax.nn.silu(sums[:, at : at + half_width]) * sums[:, at + half_width : at + 2 * half_width]
            for at in (0, 2 * half_width)
        ],
        axis=1,
    ).astype(jnp.bfloat16)
    return lax.all_gather(part_hidden, "ctx", axis=0, tiled=True)


def body(
    q_latent,
    q_rope,
    latent_keys,
    rope_keys,
    w_uv,
    moe_tokens,
    norm_gain,
    expert_ids,
    route_scale,
    w_gate,
    w_up,
    w_down,
):
    lat_piece, rope_piece = in_one_piece((latent_keys, rope_keys), "ctx", 1, 0)
    model_width = moe_tokens.shape[1] * lax.axis_size("ctx")
    half_width = w_gate.shape[2]

    tok_rows, top_count = expert_ids.shape
    expert_count = lax.axis_size("ep") // 2
    capacity = min(tok_rows, 3 * tok_rows * top_count // (2 * expert_count))
    chunk = capacity // 2
    chunk_rows = expert_count * chunk
    flat_ids = expert_ids.reshape(-1)
    onehot = (flat_ids[:, None] == jnp.arange(expert_count, dtype=jnp.int32)[None, :]).astype(
        jnp.int32
    )
    slot_index = jnp.sum((jnp.cumsum(onehot, axis=0) - onehot) * onehot, axis=1)
    target_slot = (slot_index // chunk) * chunk_rows + flat_ids * chunk + slot_index % chunk
    place_map = (
        target_slot[:, None] == jnp.arange(2 * chunk_rows, dtype=jnp.int32)[None, :]
    ).astype(jnp.float32)
    place_map = place_map.reshape(tok_rows, top_count, 2 * chunk_rows)
    route_map = jnp.sum(place_map, axis=1).astype(jnp.bfloat16)
    weight_map = jnp.sum(place_map * route_scale[:, :, None], axis=1)
    weight_high = weight_map.astype(jnp.bfloat16)
    weight_low = (weight_map - weight_high.astype(jnp.float32)).astype(jnp.bfloat16)

    with jax.named_scope("go_a"):
        rows_a = to_same_core(sent_rows(route_map[:, :chunk_rows], moe_tokens), expert_count)
    send_b = sent_rows(route_map[:, chunk_rows:], moe_tokens)
    in_w = jnp.concatenate(
        [
            w_gate[0],
            w_up[0],
            of_other_core(w_gate[0], "ep"),
            of_other_core(w_up[0], "ep"),
            jnp.zeros((w_gate.shape[1], lanes), jnp.bfloat16),
        ],
        axis=1,
    )
    down_w = jnp.concatenate([w_down[0], of_other_core(w_down[0], "ep")], axis=0)
    rows_a, send_b, in_w, down_w, lat_piece, rope_piece = lax.optimization_barrier(
        (rows_a, send_b, in_w, down_w, lat_piece, rope_piece)
    )
    with jax.named_scope("go_b"):
        rows_b = to_same_core(send_b, expert_count)
    with jax.named_scope("sum_a"):
        share_a = activation_sums(rows_a, norm_gain, in_w)
    attn_out = attention(q_latent, q_rope, lat_piece, rope_piece, w_uv)
    with jax.named_scope("sum_b"):
        share_b = activation_sums(rows_b, norm_gain, in_w)
    with jax.named_scope("act_a"):
        hidden_a = activations(share_a, model_width, half_width)
    with jax.named_scope("down_a"):
        out_a = jnp.dot(hidden_a, down_w, preferred_element_type=jnp.float32).astype(jnp.bfloat16)
    with jax.named_scope("back_a"):
        back_a = to_same_core(out_a, expert_count)
    with jax.named_scope("act_b"):
        hidden_b = activations(share_b, model_width, half_width)
    with jax.named_scope("down_b"):
        out_b = jnp.dot(hidden_b, down_w, preferred_element_type=jnp.float32).astype(jnp.bfloat16)
    with jax.named_scope("back_b"):
        back_b = to_same_core(out_b, expert_count)
    moe_out = jnp.zeros((tok_rows, moe_tokens.shape[1]), jnp.float32)
    for at, back in ((0, back_a), (chunk_rows, back_b)):
        for part in (weight_high, weight_low):
            moe_out = moe_out + jnp.dot(
                part[:, at : at + chunk_rows], back, preferred_element_type=jnp.float32
            )
    return (attn_out, moe_out.astype(jnp.bfloat16))


def solution(mesh):
    return jax.shard_map(
        body,
        mesh=mesh,
        in_specs=(
            P(("group", "ctx"), "ep"),
            P(("group", "ctx"), "ep"),
            P("group", "ctx"),
            P("group", "ctx"),
            P("ep", None, None),
            P(("group", "ep"), "ctx"),
            P("ctx"),
            P(("group", "ep"), None),
            P(("group", "ep"), None),
            P("ep", "ctx", None),
            P("ep", "ctx", None),
            P("ep", None, "ctx"),
        ),
        out_specs=(P(("group", "ctx"), "ep"), P(("group", "ep"), "ctx")),
        check_vma=False,
    )
```

```python
import jax
import jax.numpy as jnp
from jax import lax
from jax.sharding import PartitionSpec as P

score_scale = 192.0 ** (-0.5)
norm_eps = 1e-06
neg_large = -1e30
lanes = 128


def in_one_piece(arrays, axis, dim, along):
    ends, at = ([], 0)
    for a in arrays[:-1]:
        at += a.shape[along]
        ends.append(at)
    both = jnp.concatenate(arrays, axis=along)
    return tuple(jnp.split(lax.all_gather(both, axis, axis=dim, tiled=True), ends, axis=along))


def same_core(axis):
    count = lax.axis_size(axis)
    return [list(range(core, count, 2)) for core in range(2)]


def of_other_core(value, axis):
    count = lax.axis_size(axis)
    return lax.ppermute(value, axis, [(i, i ^ 1) for i in range(count)])


def attention(q_latent, q_rope, lat_piece, rope_piece, w_uv):
    seq_rows = q_latent.shape[0]
    head_count, latent_dim = w_uv.shape[:2]
    rope_dim = rope_piece.shape[0]
    query_lat = (
        q_latent.reshape(seq_rows, head_count, latent_dim)
        .transpose(1, 0, 2)
        .reshape(head_count * seq_rows, latent_dim)
    )
    query_rot = (
        q_rope.reshape(seq_rows, head_count, rope_dim)
        .transpose(1, 0, 2)
        .reshape(head_count * seq_rows, rope_dim)
    )
    query_pos = lax.axis_index("ctx") * seq_rows + jnp.tile(
        jnp.arange(seq_rows, dtype=jnp.int32), head_count
    )
    scores = jnp.dot(query_lat, lat_piece, preferred_element_type=jnp.float32)
    scores = (
        scores + jnp.dot(query_rot, rope_piece, preferred_element_type=jnp.float32)
    ) * score_scale
    key_pos = jnp.arange(lat_piece.shape[1], dtype=jnp.int32)
    visible = key_pos[None, :] <= query_pos[:, None]
    masked = jnp.where(visible, scores, neg_large)
    row_max = jnp.max(masked, axis=1, keepdims=True)
    weights = jnp.where(visible, jnp.exp(masked - row_max), 0.0)
    row_sum = jnp.sum(weights, axis=1, keepdims=True)
    update = lax.dot_general(
        weights.astype(jnp.bfloat16),
        lat_piece,
        (((1,), (1,)), ((), ())),
        preferred_element_type=jnp.float32,
    )
    context = (update / row_sum).astype(jnp.bfloat16).reshape(head_count, seq_rows, latent_dim)
    attn_heads = jnp.einsum("hsl,hlv->shv", context, w_uv, preferred_element_type=jnp.float32)
    return attn_heads.reshape(seq_rows, head_count * w_uv.shape[2]).astype(jnp.bfloat16)


def to_same_core(rows, count):
    return lax.all_to_all(
        rows.reshape(count, -1, rows.shape[1]),
        "ep",
        split_axis=0,
        concat_axis=0,
        tiled=True,
        axis_index_groups=same_core("ep"),
    ).reshape(rows.shape)


def activation_sums(rows, norm_gain, in_w):
    rows_wide = rows.astype(jnp.float32)
    row_sq = jnp.sum(rows_wide * rows_wide, axis=1, keepdims=True)
    gained = (rows_wide * norm_gain[None, :]).astype(jnp.bfloat16)
    in_part = jnp.dot(gained, in_w, preferred_element_type=jnp.float32)
    column = lax.broadcasted_iota(jnp.int32, in_part.shape, 1)
    return jnp.where(column < in_w.shape[1] - lanes, in_part, row_sq).astype(jnp.bfloat16)


def row_shares(in_part):
    return lax.psum_scatter(in_part, "ctx", scatter_dimension=0, tiled=True)


def activations(row_share, model_width, half_width):
    row_share = row_share.astype(jnp.float32)
    row_scale = lax.rsqrt(row_share[:, -1:] / model_width + norm_eps)
    sums = row_share[:, :-lanes] * row_scale
    part_hidden = jnp.concatenate(
        [
            jax.nn.silu(sums[:, at : at + half_width]) * sums[:, at + half_width : at + 2 * half_width]
            for at in (0, 2 * half_width)
        ],
        axis=1,
    ).astype(jnp.bfloat16)
    return lax.all_gather(part_hidden, "ctx", axis=0, tiled=True)


def body(
    q_latent,
    q_rope,
    latent_keys,
    rope_keys,
    w_uv,
    moe_tokens,
    norm_gain,
    expert_ids,
    route_scale,
    w_gate,
    w_up,
    w_down,
):
    model_width = moe_tokens.shape[1] * lax.axis_size("ctx")
    half_width = w_gate.shape[2]

    tok_rows, top_count = expert_ids.shape
    expert_count = lax.axis_size("ep") // 2
    capacity = min(tok_rows, 3 * tok_rows * top_count // (2 * expert_count))
    chunk = capacity // 2
    expert = jnp.arange(expert_count, dtype=jnp.int32)[:, None]
    hits = [expert == expert_ids[:, k][None, :] for k in range(top_count)]
    member = sum(hit.astype(jnp.float32) for hit in hits)
    expert_weight = sum(
        jnp.where(hit, route_scale[:, k][None, :], 0.0) for k, hit in enumerate(hits)
    )
    token = jnp.arange(tok_rows, dtype=jnp.int32)
    earlier = (token[:, None] < token[None, :]).astype(jnp.bfloat16)
    slot = jnp.dot(member.astype(jnp.bfloat16), earlier, preferred_element_type=jnp.float32)
    slot = jnp.where(member > 0.0, slot, -1.0)

    def placed(at):
        wanted = jnp.arange(at * chunk, (at + 1) * chunk, dtype=jnp.int32).astype(jnp.float32)
        return slot[:, None, :] == wanted[None, :, None]

    def sent_rows(at):
        route_map = placed(at).astype(jnp.bfloat16).reshape(expert_count * chunk, tok_rows)
        return jnp.dot(route_map, moe_tokens, preferred_element_type=jnp.float32).astype(jnp.bfloat16)

    def weighted_sum(at, back):
        weights = jnp.where(placed(at), expert_weight[:, None, :], 0.0)
        weights = weights.reshape(expert_count * chunk, tok_rows)
        high = weights.astype(jnp.bfloat16)
        low = (weights - high.astype(jnp.float32)).astype(jnp.bfloat16)
        return sum(
            lax.dot_general(part, back, (((0,), (0,)), ((), ())), preferred_element_type=jnp.float32)
            for part in (high, low)
        )

    rows_a = to_same_core(sent_rows(0), expert_count)
    send_b = sent_rows(1)
    in_w = jnp.concatenate(
        [
            w_gate[0],
            w_up[0],
            of_other_core(w_gate[0], "ep"),
            of_other_core(w_up[0], "ep"),
            jnp.zeros((w_gate.shape[1], lanes), jnp.bfloat16),
        ],
        axis=1,
    )
    down_w = jnp.concatenate([w_down[0], of_other_core(w_down[0], "ep")], axis=0)
    rows_a, send_b, in_w, down_w = lax.optimization_barrier((rows_a, send_b, in_w, down_w))
    part_a = activation_sums(rows_a, norm_gain, in_w)
    part_a, send_b = lax.optimization_barrier((part_a, send_b))
    share_a = row_shares(part_a)
    rows_b = to_same_core(send_b, expert_count)
    share_b = row_shares(activation_sums(rows_b, norm_gain, in_w))
    share_b, latent_keys, rope_keys = lax.optimization_barrier((share_b, latent_keys, rope_keys))
    lat_piece, rope_piece = in_one_piece((latent_keys, rope_keys), "ctx", 1, 0)
    attn_out = attention(q_latent, q_rope, lat_piece, rope_piece, w_uv)
    hidden_a = activations(share_a, model_width, half_width)
    out_a = jnp.dot(hidden_a, down_w, preferred_element_type=jnp.float32).astype(jnp.bfloat16)
    back_a = to_same_core(out_a, expert_count)
    hidden_b = activations(share_b, model_width, half_width)
    out_b = jnp.dot(hidden_b, down_w, preferred_element_type=jnp.float32).astype(jnp.bfloat16)
    back_b = to_same_core(out_b, expert_count)
    moe_out = (weighted_sum(0, back_a) + weighted_sum(1, back_b)).astype(jnp.bfloat16)
    return (attn_out, moe_out)


def solution(mesh):
    return jax.shard_map(
        body,
        mesh=mesh,
        in_specs=(
            P(("group", "ctx"), "ep"),
            P(("group", "ctx"), "ep"),
            P("group", "ctx"),
            P("group", "ctx"),
            P("ep", None, None),
            P(("group", "ep"), "ctx"),
            P("ctx"),
            P(("group", "ep"), None),
            P(("group", "ep"), None),
            P("ep", "ctx", None),
            P("ep", "ctx", None),
            P("ep", None, "ctx"),
        ),
        out_specs=(P(("group", "ctx"), "ep"), P(("group", "ep"), "ctx")),
        check_vma=False,
    )
```

```python
import jax
import jax.numpy as jnp
from jax import lax
from jax.experimental import pallas as pl
from jax.experimental.pallas import tpu as pltpu
from jax.sharding import PartitionSpec as P

score_scale = 192.0 ** (-0.5)
norm_eps = 1e-06
neg_large = -1e30
lanes = 128


def in_one_piece(arrays, axis, dim, along):
    ends, at = ([], 0)
    for a in arrays[:-1]:
        at += a.shape[along]
        ends.append(at)
    both = jnp.concatenate(arrays, axis=along)
    return tuple(jnp.split(lax.all_gather(both, axis, axis=dim, tiled=True), ends, axis=along))


def same_core(axis):
    count = lax.axis_size(axis)
    return [list(range(core, count, 2)) for core in range(2)]


def of_other_core(value, axis):
    count = lax.axis_size(axis)
    return lax.ppermute(value, axis, [(i, i ^ 1) for i in range(count)])


def attention(q_latent, q_rope, lat_piece, rope_piece, w_uv):
    seq_rows = q_latent.shape[0]
    head_count, latent_dim = w_uv.shape[:2]
    rope_dim = rope_piece.shape[0]
    query_lat = (
        q_latent.reshape(seq_rows, head_count, latent_dim)
        .transpose(1, 0, 2)
        .reshape(head_count * seq_rows, latent_dim)
    )
    query_rot = (
        q_rope.reshape(seq_rows, head_count, rope_dim)
        .transpose(1, 0, 2)
        .reshape(head_count * seq_rows, rope_dim)
    )
    query_pos = lax.axis_index("ctx") * seq_rows + jnp.tile(
        jnp.arange(seq_rows, dtype=jnp.int32), head_count
    )
    scores = jnp.dot(query_lat, lat_piece, preferred_element_type=jnp.float32)
    scores = (
        scores + jnp.dot(query_rot, rope_piece, preferred_element_type=jnp.float32)
    ) * score_scale
    key_pos = jnp.arange(lat_piece.shape[1], dtype=jnp.int32)
    visible = key_pos[None, :] <= query_pos[:, None]
    masked = jnp.where(visible, scores, neg_large)
    row_max = jnp.max(masked, axis=1, keepdims=True)
    weights = jnp.where(visible, jnp.exp(masked - row_max), 0.0)
    row_sum = jnp.sum(weights, axis=1, keepdims=True)
    update = lax.dot_general(
        weights.astype(jnp.bfloat16),
        lat_piece,
        (((1,), (1,)), ((), ())),
        preferred_element_type=jnp.float32,
    )
    context = (update / row_sum).astype(jnp.bfloat16).reshape(head_count, seq_rows, latent_dim)
    attn_heads = jnp.einsum("hsl,hlv->shv", context, w_uv, preferred_element_type=jnp.float32)
    return attn_heads.reshape(seq_rows, head_count * w_uv.shape[2]).astype(jnp.bfloat16)


def to_same_core(rows, count):
    return lax.all_to_all(
        rows.reshape(count, -1, rows.shape[1]),
        "ep",
        split_axis=0,
        concat_axis=0,
        tiled=True,
        axis_index_groups=same_core("ep"),
    ).reshape(rows.shape)


def sums_kernel(rows, gain, *refs):
    count = len(refs) - 6
    weights, out = refs[:count], refs[count]
    gained, fetched, sums, fetch_done, store_done = refs[count + 1 :]
    width = fetched.shape[2]
    fetches = [
        pltpu.make_async_copy(weights[i], fetched.at[i], fetch_done.at[i]) for i in range(count)
    ]
    for fetch in fetches:
        fetch.start()
    rows_wide = rows[...].astype(jnp.float32)
    gained[...] = (rows_wide * gain[...]).astype(jnp.bfloat16)
    row_sq = jnp.sum(rows_wide * rows_wide, axis=1, keepdims=True)
    sums[:, count * width :] = jnp.broadcast_to(row_sq, (rows.shape[0], lanes)).astype(jnp.bfloat16)
    ends = [(i + 1) * width for i in range(count - 1)] + [sums.shape[1]]
    stores = []
    for i in range(count):
        fetches[i].wait()
        sums[:, i * width : (i + 1) * width] = jnp.dot(
            gained[...], fetched[i], preferred_element_type=jnp.float32
        ).astype(jnp.bfloat16)
        piece = pl.ds(i * width, ends[i] - i * width)
        store = pltpu.make_async_copy(sums.at[:, piece], out.at[:, piece], store_done.at[i])
        store.start()
        stores.append(store)
    for store in stores:
        store.wait()


def activation_sums(rows, norm_gain, weights):
    row_count, width = rows.shape
    block = weights[0].shape[1]
    count = len(weights)
    columns = count * block + lanes
    return pl.pallas_call(
        sums_kernel,
        out_shape=jax.ShapeDtypeStruct((row_count, columns), jnp.bfloat16),
        in_specs=[
            pl.BlockSpec(memory_space=pltpu.VMEM),
            pl.BlockSpec(memory_space=pltpu.VMEM),
            *[pl.BlockSpec(memory_space=pl.ANY) for _ in weights],
        ],
        out_specs=pl.BlockSpec(memory_space=pl.ANY),
        scratch_shapes=[
            pltpu.VMEM((row_count, width), jnp.bfloat16),
            pltpu.VMEM((count, width, block), jnp.bfloat16),
            pltpu.VMEM((row_count, columns), jnp.bfloat16),
            pltpu.SemaphoreType.DMA((count,)),
            pltpu.SemaphoreType.DMA((count,)),
        ],
        cost_estimate=pl.CostEstimate(
            flops=2 * row_count * width * count * block,
            bytes_accessed=2 * (row_count * (width + columns) + count * width * block),
            transcendentals=0,
        ),
        name="gate_up_sums",
    )(rows, norm_gain[None, :], *weights)


def row_shares(in_part):
    return lax.psum_scatter(in_part, "ctx", scatter_dimension=0, tiled=True)


def activations(row_share, model_width, half_width):
    row_share = row_share.astype(jnp.float32)
    row_scale = lax.rsqrt(row_share[:, -1:] / model_width + norm_eps)
    sums = row_share[:, :-lanes] * row_scale
    part_hidden = jnp.concatenate(
        [
            jax.nn.silu(sums[:, at : at + half_width]) * sums[:, at + half_width : at + 2 * half_width]
            for at in (0, 2 * half_width)
        ],
        axis=1,
    ).astype(jnp.bfloat16)
    return lax.all_gather(part_hidden, "ctx", axis=0, tiled=True)


def body(
    q_latent,
    q_rope,
    latent_keys,
    rope_keys,
    w_uv,
    moe_tokens,
    norm_gain,
    expert_ids,
    route_scale,
    w_gate,
    w_up,
    w_down,
):
    lat_piece, rope_piece = in_one_piece((latent_keys, rope_keys), "ctx", 1, 0)
    model_width = moe_tokens.shape[1] * lax.axis_size("ctx")
    half_width = w_gate.shape[2]

    tok_rows, top_count = expert_ids.shape
    expert_count = lax.axis_size("ep") // 2
    capacity = min(tok_rows, 3 * tok_rows * top_count // (2 * expert_count))
    chunk = capacity // 2
    expert = jnp.arange(expert_count, dtype=jnp.int32)[:, None]
    hits = [expert == expert_ids[:, k][None, :] for k in range(top_count)]
    member = sum(hit.astype(jnp.float32) for hit in hits)
    expert_weight = sum(
        jnp.where(hit, route_scale[:, k][None, :], 0.0) for k, hit in enumerate(hits)
    )
    token = jnp.arange(tok_rows, dtype=jnp.int32)
    earlier = (token[:, None] < token[None, :]).astype(jnp.bfloat16)
    slot = jnp.dot(member.astype(jnp.bfloat16), earlier, preferred_element_type=jnp.float32)
    slot = jnp.where(member > 0.0, slot, -1.0)

    def placed(at):
        wanted = jnp.arange(at * chunk, (at + 1) * chunk, dtype=jnp.int32).astype(jnp.float32)
        return slot[:, None, :] == wanted[None, :, None]

    def sent_rows(at):
        route_map = placed(at).astype(jnp.bfloat16).reshape(expert_count * chunk, tok_rows)
        return jnp.dot(route_map, moe_tokens, preferred_element_type=jnp.float32).astype(jnp.bfloat16)

    def weighted_sum(at, back):
        weights = jnp.where(placed(at), expert_weight[:, None, :], 0.0)
        weights = weights.reshape(expert_count * chunk, tok_rows)
        high = weights.astype(jnp.bfloat16)
        low = (weights - high.astype(jnp.float32)).astype(jnp.bfloat16)
        return sum(
            lax.dot_general(part, back, (((0,), (0,)), ((), ())), preferred_element_type=jnp.float32)
            for part in (high, low)
        )

    rows_a = to_same_core(sent_rows(0), expert_count)
    send_b = sent_rows(1)
    in_w = (w_gate[0], w_up[0], of_other_core(w_gate[0], "ep"), of_other_core(w_up[0], "ep"))
    down_w = jnp.concatenate([w_down[0], of_other_core(w_down[0], "ep")], axis=0)
    rows_a, send_b, in_w, down_w = lax.optimization_barrier((rows_a, send_b, in_w, down_w))
    part_a = activation_sums(rows_a, norm_gain, in_w)
    part_a, send_b = lax.optimization_barrier((part_a, send_b))
    share_a = row_shares(part_a)
    rows_b = to_same_core(send_b, expert_count)
    share_b = row_shares(activation_sums(rows_b, norm_gain, in_w))
    attn_out = attention(q_latent, q_rope, lat_piece, rope_piece, w_uv)
    hidden_a = activations(share_a, model_width, half_width)
    out_a = jnp.dot(hidden_a, down_w, preferred_element_type=jnp.float32).astype(jnp.bfloat16)
    back_a = to_same_core(out_a, expert_count)
    hidden_b = activations(share_b, model_width, half_width)
    out_b = jnp.dot(hidden_b, down_w, preferred_element_type=jnp.float32).astype(jnp.bfloat16)
    back_b = to_same_core(out_b, expert_count)
    moe_out = (weighted_sum(0, back_a) + weighted_sum(1, back_b)).astype(jnp.bfloat16)
    return (attn_out, moe_out)


def solution(mesh):
    return jax.shard_map(
        body,
        mesh=mesh,
        in_specs=(
            P(("group", "ctx"), "ep"),
            P(("group", "ctx"), "ep"),
            P("group", "ctx"),
            P("group", "ctx"),
            P("ep", None, None),
            P(("group", "ep"), "ctx"),
            P("ctx"),
            P(("group", "ep"), None),
            P(("group", "ep"), None),
            P("ep", "ctx", None),
            P("ep", "ctx", None),
            P("ep", None, "ctx"),
        ),
        out_specs=(P(("group", "ctx"), "ep"), P(("group", "ep"), "ctx")),
        check_vma=False,
    )
```

```python
import jax
import jax.numpy as jnp
from jax import lax
from jax.experimental import pallas as pl
from jax.experimental.pallas import tpu as pltpu
from jax.sharding import PartitionSpec as P

score_scale = 192.0 ** (-0.5)
norm_eps = 1e-06
neg_large = -1e30
lanes = 128


def in_one_piece(arrays, axis, dim, along):
    ends, at = ([], 0)
    for a in arrays[:-1]:
        at += a.shape[along]
        ends.append(at)
    both = jnp.concatenate(arrays, axis=along)
    return tuple(jnp.split(lax.all_gather(both, axis, axis=dim, tiled=True), ends, axis=along))


def same_core(axis):
    count = lax.axis_size(axis)
    return [list(range(core, count, 2)) for core in range(2)]


def of_other_core(value, axis):
    count = lax.axis_size(axis)
    return lax.ppermute(value, axis, [(i, i ^ 1) for i in range(count)])


def attention(q_latent, q_rope, lat_piece, rope_piece, w_uv):
    seq_rows = q_latent.shape[0]
    head_count, latent_dim = w_uv.shape[:2]
    rope_dim = rope_piece.shape[0]
    query_lat = (
        q_latent.reshape(seq_rows, head_count, latent_dim)
        .transpose(1, 0, 2)
        .reshape(head_count * seq_rows, latent_dim)
    )
    query_rot = (
        q_rope.reshape(seq_rows, head_count, rope_dim)
        .transpose(1, 0, 2)
        .reshape(head_count * seq_rows, rope_dim)
    )
    query_pos = lax.axis_index("ctx") * seq_rows + jnp.tile(
        jnp.arange(seq_rows, dtype=jnp.int32), head_count
    )
    scores = jnp.dot(query_lat, lat_piece, preferred_element_type=jnp.float32)
    scores = (
        scores + jnp.dot(query_rot, rope_piece, preferred_element_type=jnp.float32)
    ) * score_scale
    key_pos = jnp.arange(lat_piece.shape[1], dtype=jnp.int32)
    visible = key_pos[None, :] <= query_pos[:, None]
    masked = jnp.where(visible, scores, neg_large)
    row_max = jnp.max(masked, axis=1, keepdims=True)
    weights = jnp.where(visible, jnp.exp(masked - row_max), 0.0)
    row_sum = jnp.sum(weights, axis=1, keepdims=True)
    update = lax.dot_general(
        weights.astype(jnp.bfloat16),
        lat_piece,
        (((1,), (1,)), ((), ())),
        preferred_element_type=jnp.float32,
    )
    context = (update / row_sum).astype(jnp.bfloat16).reshape(head_count, seq_rows, latent_dim)
    attn_heads = jnp.einsum("hsl,hlv->shv", context, w_uv, preferred_element_type=jnp.float32)
    return attn_heads.reshape(seq_rows, head_count * w_uv.shape[2]).astype(jnp.bfloat16)


def to_same_core(rows, count):
    return lax.all_to_all(
        rows.reshape(count, -1, rows.shape[1]),
        "ep",
        split_axis=0,
        concat_axis=0,
        tiled=True,
        axis_index_groups=same_core("ep"),
    ).reshape(rows.shape)


def sums_kernel(rows, gain, *refs):
    count = len(refs) - 7
    weights, out = refs[:count], refs[count]
    taken, gained, fetched, sums, fetch_done, store_done = refs[count + 1 :]
    width = fetched.shape[2]
    fetches = [
        pltpu.make_async_copy(weights[i], fetched.at[i], fetch_done.at[i]) for i in range(count)
    ]
    take = pltpu.make_async_copy(rows, taken, fetch_done.at[count])
    take.start()
    for fetch in fetches:
        fetch.start()
    take.wait()
    rows_wide = taken[...].astype(jnp.float32)
    gained[...] = (rows_wide * gain[...]).astype(jnp.bfloat16)
    row_sq = jnp.sum(rows_wide * rows_wide, axis=1, keepdims=True)
    sums[:, count * width :] = jnp.broadcast_to(row_sq, (taken.shape[0], lanes)).astype(jnp.bfloat16)
    ends = [(i + 1) * width for i in range(count - 1)] + [sums.shape[1]]
    stores = []
    for i in range(count):
        fetches[i].wait()
        sums[:, i * width : (i + 1) * width] = jnp.dot(
            gained[...], fetched[i], preferred_element_type=jnp.float32
        ).astype(jnp.bfloat16)
        piece = pl.ds(i * width, ends[i] - i * width)
        store = pltpu.make_async_copy(sums.at[:, piece], out.at[:, piece], store_done.at[i])
        store.start()
        stores.append(store)
    for store in stores:
        store.wait()


def activation_sums(rows, norm_gain, weights):
    row_count, width = rows.shape
    block = weights[0].shape[1]
    count = len(weights)
    columns = count * block + lanes
    return pl.pallas_call(
        sums_kernel,
        out_shape=jax.ShapeDtypeStruct((row_count, columns), jnp.bfloat16),
        in_specs=[
            pl.BlockSpec(memory_space=pl.ANY),
            pl.BlockSpec(memory_space=pltpu.VMEM),
            *[pl.BlockSpec(memory_space=pl.ANY) for _ in weights],
        ],
        out_specs=pl.BlockSpec(memory_space=pl.ANY),
        scratch_shapes=[
            pltpu.VMEM((row_count, width), jnp.bfloat16),
            pltpu.VMEM((row_count, width), jnp.bfloat16),
            pltpu.VMEM((count, width, block), jnp.bfloat16),
            pltpu.VMEM((row_count, columns), jnp.bfloat16),
            pltpu.SemaphoreType.DMA((count + 1,)),
            pltpu.SemaphoreType.DMA((count,)),
        ],
        cost_estimate=pl.CostEstimate(
            flops=2 * row_count * width * count * block,
            bytes_accessed=2 * (row_count * (width + columns) + count * width * block),
            transcendentals=0,
        ),
        name="gate_up_sums",
    )(rows, norm_gain[None, :], *weights)


def row_shares(in_part):
    return lax.psum_scatter(in_part, "ctx", scatter_dimension=0, tiled=True)


def activations(row_share, model_width, half_width):
    row_share = row_share.astype(jnp.float32)
    row_scale = lax.rsqrt(row_share[:, -1:] / model_width + norm_eps)
    sums = row_share[:, :-lanes] * row_scale
    part_hidden = jnp.concatenate(
        [
            jax.nn.silu(sums[:, at : at + half_width]) * sums[:, at + half_width : at + 2 * half_width]
            for at in (0, 2 * half_width)
        ],
        axis=1,
    ).astype(jnp.bfloat16)
    return lax.all_gather(part_hidden, "ctx", axis=0, tiled=True)


def body(
    q_latent,
    q_rope,
    latent_keys,
    rope_keys,
    w_uv,
    moe_tokens,
    norm_gain,
    expert_ids,
    route_scale,
    w_gate,
    w_up,
    w_down,
):
    model_width = moe_tokens.shape[1] * lax.axis_size("ctx")
    half_width = w_gate.shape[2]

    tok_rows, top_count = expert_ids.shape
    expert_count = lax.axis_size("ep") // 2
    capacity = min(tok_rows, 3 * tok_rows * top_count // (2 * expert_count))
    chunk = capacity // 2
    expert = jnp.arange(expert_count, dtype=jnp.int32)[:, None]
    hits = [expert == expert_ids[:, k][None, :] for k in range(top_count)]
    member = sum(hit.astype(jnp.float32) for hit in hits)
    expert_weight = sum(
        jnp.where(hit, route_scale[:, k][None, :], 0.0) for k, hit in enumerate(hits)
    )
    token = jnp.arange(tok_rows, dtype=jnp.int32)
    earlier = (token[:, None] < token[None, :]).astype(jnp.bfloat16)
    slot = jnp.dot(member.astype(jnp.bfloat16), earlier, preferred_element_type=jnp.float32)
    slot = jnp.where(member > 0.0, slot, -1.0)

    def placed(at):
        wanted = jnp.arange(at * chunk, (at + 1) * chunk, dtype=jnp.int32).astype(jnp.float32)
        return slot[:, None, :] == wanted[None, :, None]

    def sent_rows(at):
        route_map = placed(at).astype(jnp.bfloat16).reshape(expert_count * chunk, tok_rows)
        return jnp.dot(route_map, moe_tokens, preferred_element_type=jnp.float32).astype(jnp.bfloat16)

    def weighted_sum(at, back):
        weights = jnp.where(placed(at), expert_weight[:, None, :], 0.0)
        weights = weights.reshape(expert_count * chunk, tok_rows)
        high = weights.astype(jnp.bfloat16)
        low = (weights - high.astype(jnp.float32)).astype(jnp.bfloat16)
        return sum(
            lax.dot_general(part, back, (((0,), (0,)), ((), ())), preferred_element_type=jnp.float32)
            for part in (high, low)
        )

    rows_a = to_same_core(sent_rows(0), expert_count)
    send_b = sent_rows(1)
    in_w = (w_gate[0], w_up[0], of_other_core(w_gate[0], "ep"), of_other_core(w_up[0], "ep"))
    down_w = jnp.concatenate([w_down[0], of_other_core(w_down[0], "ep")], axis=0)
    rows_a, send_b, in_w, down_w = lax.optimization_barrier((rows_a, send_b, in_w, down_w))
    rows_b = to_same_core(send_b, expert_count)
    share_a = row_shares(activation_sums(rows_a, norm_gain, in_w))
    share_b = row_shares(activation_sums(rows_b, norm_gain, in_w))
    share_b, latent_keys, rope_keys = lax.optimization_barrier((share_b, latent_keys, rope_keys))
    lat_piece, rope_piece = in_one_piece((latent_keys, rope_keys), "ctx", 1, 0)
    attn_out = attention(q_latent, q_rope, lat_piece, rope_piece, w_uv)
    hidden_a = activations(share_a, model_width, half_width)
    out_a = jnp.dot(hidden_a, down_w, preferred_element_type=jnp.float32).astype(jnp.bfloat16)
    back_a = to_same_core(out_a, expert_count)
    hidden_b = activations(share_b, model_width, half_width)
    out_b = jnp.dot(hidden_b, down_w, preferred_element_type=jnp.float32).astype(jnp.bfloat16)
    back_b = to_same_core(out_b, expert_count)
    moe_out = (weighted_sum(0, back_a) + weighted_sum(1, back_b)).astype(jnp.bfloat16)
    return (attn_out, moe_out)


def solution(mesh):
    return jax.shard_map(
        body,
        mesh=mesh,
        in_specs=(
            P(("group", "ctx"), "ep"),
            P(("group", "ctx"), "ep"),
            P("group", "ctx"),
            P("group", "ctx"),
            P("ep", None, None),
            P(("group", "ep"), "ctx"),
            P("ctx"),
            P(("group", "ep"), None),
            P(("group", "ep"), None),
            P("ep", "ctx", None),
            P("ep", "ctx", None),
            P("ep", None, "ctx"),
        ),
        out_specs=(P(("group", "ctx"), "ep"), P(("group", "ep"), "ctx")),
        check_vma=False,
    )
```

```python
import jax
import jax.numpy as jnp
from jax import lax
from jax.sharding import PartitionSpec as P

score_scale = 192.0 ** (-0.5)
norm_eps = 1e-06
neg_large = -1e30
lanes = 128


def same_core(axis):
    count = lax.axis_size(axis)
    return [list(range(core, count, 2)) for core in range(2)]


def of_other_core(value, axis):
    count = lax.axis_size(axis)
    return lax.ppermute(value, axis, [(i, i ^ 1) for i in range(count)])


def attention(q_latent, q_rope, lat_piece, rope_piece, w_uv):
    seq_rows = q_latent.shape[0]
    head_count, latent_dim = w_uv.shape[:2]
    rope_dim = rope_piece.shape[0]
    query_lat = (
        q_latent.reshape(seq_rows, head_count, latent_dim)
        .transpose(1, 0, 2)
        .reshape(head_count * seq_rows, latent_dim)
    )
    query_rot = (
        q_rope.reshape(seq_rows, head_count, rope_dim)
        .transpose(1, 0, 2)
        .reshape(head_count * seq_rows, rope_dim)
    )
    query_pos = lax.axis_index("ctx") * seq_rows + jnp.tile(
        jnp.arange(seq_rows, dtype=jnp.int32), head_count
    )
    scores = jnp.dot(query_lat, lat_piece, preferred_element_type=jnp.float32)
    scores = (
        scores + jnp.dot(query_rot, rope_piece, preferred_element_type=jnp.float32)
    ) * score_scale
    key_pos = jnp.arange(lat_piece.shape[1], dtype=jnp.int32)
    visible = key_pos[None, :] <= query_pos[:, None]
    masked = jnp.where(visible, scores, neg_large)
    row_max = jnp.max(masked, axis=1, keepdims=True)
    weights = jnp.where(visible, jnp.exp(masked - row_max), 0.0)
    row_sum = jnp.sum(weights, axis=1, keepdims=True)
    update = lax.dot_general(
        weights.astype(jnp.bfloat16),
        lat_piece,
        (((1,), (1,)), ((), ())),
        preferred_element_type=jnp.float32,
    )
    context = (update / row_sum).astype(jnp.bfloat16).reshape(head_count, seq_rows, latent_dim)
    attn_heads = jnp.einsum("hsl,hlv->shv", context, w_uv, preferred_element_type=jnp.float32)
    return attn_heads.reshape(seq_rows, head_count * w_uv.shape[2]).astype(jnp.bfloat16)


def to_same_core(rows, count):
    return lax.all_to_all(
        rows.reshape(count, -1, rows.shape[1]),
        "ep",
        split_axis=0,
        concat_axis=0,
        tiled=True,
        axis_index_groups=same_core("ep"),
    ).reshape(rows.shape)


def activation_sums(rows, norm_gain, in_w):
    rows_wide = rows.astype(jnp.float32)
    row_sq = jnp.sum(rows_wide * rows_wide, axis=1, keepdims=True)
    gained = (rows_wide * norm_gain[None, :]).astype(jnp.bfloat16)
    in_part = jnp.dot(gained, in_w, preferred_element_type=jnp.float32)
    column = lax.broadcasted_iota(jnp.int32, in_part.shape, 1)
    return jnp.where(column < in_w.shape[1] - lanes, in_part, row_sq).astype(jnp.bfloat16)


def row_shares(in_part):
    return lax.psum_scatter(in_part, "ctx", scatter_dimension=0, tiled=True)


def activations(row_share, model_width):
    width = (row_share.shape[1] - lanes) // 2
    row_scale = lax.rsqrt(row_share[:, -1:].astype(jnp.float32) / model_width + norm_eps)
    gate = row_share[:, :width].astype(jnp.float32) * row_scale
    up = row_share[:, width : 2 * width].astype(jnp.float32) * row_scale
    part_hidden = (jax.nn.silu(gate) * up).astype(jnp.bfloat16)
    return lax.all_gather(part_hidden, "ctx", axis=0, tiled=True)


def body(
    q_latent,
    q_rope,
    latent_keys,
    rope_keys,
    w_uv,
    moe_tokens,
    norm_gain,
    expert_ids,
    route_scale,
    w_gate,
    w_up,
    w_down,
):
    model_width = moe_tokens.shape[1] * lax.axis_size("ctx")

    tok_rows, top_count = expert_ids.shape
    expert_count = lax.axis_size("ep") // 2
    capacity = min(tok_rows, 3 * tok_rows * top_count // (2 * expert_count))
    chunk = capacity // 2
    expert = jnp.arange(expert_count, dtype=jnp.int32)[:, None]
    hits = [expert == expert_ids[:, k][None, :] for k in range(top_count)]
    member = sum(hit.astype(jnp.float32) for hit in hits)
    expert_weight = sum(
        jnp.where(hit, route_scale[:, k][None, :], 0.0) for k, hit in enumerate(hits)
    )
    token = jnp.arange(tok_rows, dtype=jnp.int32)
    earlier = (token[:, None] < token[None, :]).astype(jnp.bfloat16)
    slot = jnp.dot(member.astype(jnp.bfloat16), earlier, preferred_element_type=jnp.float32)
    slot = jnp.where(member > 0.0, slot, -1.0)

    def placed(slots, at):
        wanted = jnp.arange(at * chunk, (at + 1) * chunk, dtype=jnp.int32).astype(jnp.float32)
        return slots[:, None, :] == wanted[None, :, None]

    def sent_rows(slots, at):
        route_map = jnp.where(placed(slots, at), 1.0, 0.0).astype(jnp.bfloat16)
        route_map = route_map.reshape(expert_count * chunk, tok_rows)
        return jnp.dot(route_map, moe_tokens, preferred_element_type=jnp.float32).astype(jnp.bfloat16)

    def return_weights(slots, at):
        weights = jnp.where(placed(slots, at), expert_weight[:, None, :], 0.0).astype(jnp.bfloat16)
        return weights.reshape(expert_count * chunk, tok_rows).T

    rows_a = to_same_core(sent_rows(slot, 0), expert_count)
    slot_b, slot_back = lax.optimization_barrier((slot, slot))
    send_b = sent_rows(slot_b, 1)
    in_w = jnp.concatenate(
        [
            w_gate[0],
            of_other_core(w_gate[0], "ep"),
            w_up[0],
            of_other_core(w_up[0], "ep"),
            jnp.zeros((w_gate.shape[1], lanes), jnp.bfloat16),
        ],
        axis=1,
    )
    down_w = jnp.concatenate([w_down[0], of_other_core(w_down[0], "ep")], axis=0)
    weights_a, weights_b = (return_weights(slot_back, at) for at in range(2))
    own_keys = jnp.concatenate([latent_keys, rope_keys], axis=0)
    rows_a, send_b, in_w, down_w, weights_a, weights_b, own_keys = lax.optimization_barrier(
        (rows_a, send_b, in_w, down_w, weights_a, weights_b, own_keys)
    )
    part_a = activation_sums(rows_a, norm_gain, in_w)
    part_a, send_b = lax.optimization_barrier((part_a, send_b))
    share_a = row_shares(part_a)
    rows_b = to_same_core(send_b, expert_count)
    share_b = row_shares(activation_sums(rows_b, norm_gain, in_w))
    share_b, own_keys = lax.optimization_barrier((share_b, own_keys))
    all_keys = lax.all_gather(own_keys, "ctx", axis=1, tiled=True)
    lat_piece, rope_piece = jnp.split(all_keys, [latent_keys.shape[0]], axis=0)
    attn_out = attention(q_latent, q_rope, lat_piece, rope_piece, w_uv)
    hidden_a = activations(share_a, model_width)
    out_a = jnp.dot(hidden_a, down_w, preferred_element_type=jnp.float32).astype(jnp.bfloat16)
    back_a = to_same_core(out_a, expert_count)
    hidden_b = activations(share_b, model_width)
    out_b = jnp.dot(hidden_b, down_w, preferred_element_type=jnp.float32).astype(jnp.bfloat16)
    back_b = to_same_core(out_b, expert_count)
    mixed = jnp.dot(weights_a, back_a, preferred_element_type=jnp.float32)
    moe_out = mixed + jnp.dot(weights_b, back_b, preferred_element_type=jnp.float32)
    moe_out = moe_out.astype(jnp.bfloat16)
    return (attn_out, moe_out)


def solution(mesh):
    return jax.shard_map(
        body,
        mesh=mesh,
        in_specs=(
            P(("group", "ctx"), "ep"),
            P(("group", "ctx"), "ep"),
            P("group", "ctx"),
            P("group", "ctx"),
            P("ep", None, None),
            P(("group", "ep"), "ctx"),
            P("ctx"),
            P(("group", "ep"), None),
            P(("group", "ep"), None),
            P("ep", "ctx", None),
            P("ep", "ctx", None),
            P("ep", None, "ctx"),
        ),
        out_specs=(P(("group", "ctx"), "ep"), P(("group", "ep"), "ctx")),
        check_vma=False,
    )
```

```python
import jax
import jax.numpy as jnp
from jax import lax
from jax.sharding import PartitionSpec as P

score_scale = 192.0 ** (-0.5)
norm_eps = 1e-06
neg_large = -1e30
lanes = 128


def one_core_each(axis):
    chips = range(lax.axis_size(axis) // 2)
    return [[2 * chip + (chip + turn) % 2 for chip in chips] for turn in range(2)]


def of_other_core(value, axis):
    count = lax.axis_size(axis)
    return lax.ppermute(value, axis, [(i, i ^ 1) for i in range(count)])


def attention(q_latent, q_rope, lat_piece, rope_piece, w_uv):
    seq_rows = q_latent.shape[0]
    head_count, latent_dim = w_uv.shape[:2]
    rope_dim = rope_piece.shape[0]
    query_lat = (
        q_latent.reshape(seq_rows, head_count, latent_dim)
        .transpose(1, 0, 2)
        .reshape(head_count * seq_rows, latent_dim)
    )
    query_rot = (
        q_rope.reshape(seq_rows, head_count, rope_dim)
        .transpose(1, 0, 2)
        .reshape(head_count * seq_rows, rope_dim)
    )
    query_pos = lax.axis_index("ctx") * seq_rows + jnp.tile(
        jnp.arange(seq_rows, dtype=jnp.int32), head_count
    )
    scores = jnp.dot(query_lat, lat_piece, preferred_element_type=jnp.float32)
    scores = (
        scores + jnp.dot(query_rot, rope_piece, preferred_element_type=jnp.float32)
    ) * score_scale
    key_pos = jnp.arange(lat_piece.shape[1], dtype=jnp.int32)
    visible = key_pos[None, :] <= query_pos[:, None]
    masked = jnp.where(visible, scores, neg_large)
    row_max = jnp.max(masked, axis=1, keepdims=True)
    weights = jnp.where(visible, jnp.exp(masked - row_max), 0.0)
    row_sum = jnp.sum(weights, axis=1, keepdims=True)
    update = lax.dot_general(
        weights.astype(jnp.bfloat16),
        lat_piece,
        (((1,), (1,)), ((), ())),
        preferred_element_type=jnp.float32,
    )
    context = (update / row_sum).astype(jnp.bfloat16).reshape(head_count, seq_rows, latent_dim)
    attn_heads = jnp.einsum("hsl,hlv->shv", context, w_uv, preferred_element_type=jnp.float32)
    return attn_heads.reshape(seq_rows, head_count * w_uv.shape[2]).astype(jnp.bfloat16)


def to_group(rows, count):
    return lax.all_to_all(
        rows.reshape(count, -1, rows.shape[1]),
        "ep",
        split_axis=0,
        concat_axis=0,
        tiled=True,
        axis_index_groups=one_core_each("ep"),
    ).reshape(rows.shape)


def activation_sums(rows, norm_gain, in_w):
    rows_wide = rows.astype(jnp.float32)
    row_sq = jnp.sum(rows_wide * rows_wide, axis=1, keepdims=True)
    gained = (rows_wide * norm_gain[None, :]).astype(jnp.bfloat16)
    in_part = jnp.dot(gained, in_w, preferred_element_type=jnp.float32)
    column = lax.broadcasted_iota(jnp.int32, in_part.shape, 1)
    return jnp.where(column < in_w.shape[1] - lanes, in_part, row_sq).astype(jnp.bfloat16)


def row_shares(in_part):
    return lax.psum_scatter(in_part, "ctx", scatter_dimension=0, tiled=True)


def activations(row_share, model_width):
    width = (row_share.shape[1] - lanes) // 2
    row_scale = lax.rsqrt(row_share[:, -1:].astype(jnp.float32) / model_width + norm_eps)
    gate = row_share[:, :width].astype(jnp.float32) * row_scale
    up = row_share[:, width : 2 * width].astype(jnp.float32) * row_scale
    part_hidden = (jax.nn.silu(gate) * up).astype(jnp.bfloat16)
    return lax.all_gather(part_hidden, "ctx", axis=0, tiled=True)


def body(
    q_latent,
    q_rope,
    latent_keys,
    rope_keys,
    w_uv,
    moe_tokens,
    norm_gain,
    expert_ids,
    route_scale,
    w_gate,
    w_up,
    w_down,
):
    model_width = moe_tokens.shape[1] * lax.axis_size("ctx")

    tok_rows, top_count = expert_ids.shape
    expert_count = lax.axis_size("ep") // 2
    capacity = min(tok_rows, 3 * tok_rows * top_count // (2 * expert_count))
    chunk = capacity // 2
    expert = jnp.arange(expert_count, dtype=jnp.int32)[:, None]
    hits = [expert == expert_ids[:, k][None, :] for k in range(top_count)]
    member = sum(hit.astype(jnp.float32) for hit in hits)
    expert_weight = sum(
        jnp.where(hit, route_scale[:, k][None, :], 0.0) for k, hit in enumerate(hits)
    )
    token = jnp.arange(tok_rows, dtype=jnp.int32)
    earlier = (token[:, None] < token[None, :]).astype(jnp.bfloat16)
    slot = jnp.dot(member.astype(jnp.bfloat16), earlier, preferred_element_type=jnp.float32)
    slot = jnp.where(member > 0.0, slot, -1.0)

    def placed(slots, at):
        wanted = jnp.arange(at * chunk, (at + 1) * chunk, dtype=jnp.int32).astype(jnp.float32)
        return slots[:, None, :] == wanted[None, :, None]

    def sent_rows(slots, at):
        route_map = jnp.where(placed(slots, at), 1.0, 0.0).astype(jnp.bfloat16)
        route_map = route_map.reshape(expert_count * chunk, tok_rows)
        return jnp.dot(route_map, moe_tokens, preferred_element_type=jnp.float32).astype(jnp.bfloat16)

    def return_weights(slots, at):
        weights = jnp.where(placed(slots, at), expert_weight[:, None, :], 0.0).astype(jnp.bfloat16)
        return weights.reshape(expert_count * chunk, tok_rows).T

    rows_a = to_group(sent_rows(slot, 0), expert_count)
    slot_b, slot_back = lax.optimization_barrier((slot, slot))
    send_b = sent_rows(slot_b, 1)
    in_w = jnp.concatenate(
        [
            w_gate[0],
            of_other_core(w_gate[0], "ep"),
            w_up[0],
            of_other_core(w_up[0], "ep"),
            jnp.zeros((w_gate.shape[1], lanes), jnp.bfloat16),
        ],
        axis=1,
    )
    down_w = jnp.concatenate([w_down[0], of_other_core(w_down[0], "ep")], axis=0)
    weights_a, weights_b = (return_weights(slot_back, at) for at in range(2))
    own_keys = jnp.concatenate([latent_keys, rope_keys], axis=0)
    rows_a, send_b, in_w, down_w, weights_a, weights_b, own_keys = lax.optimization_barrier(
        (rows_a, send_b, in_w, down_w, weights_a, weights_b, own_keys)
    )
    part_a = activation_sums(rows_a, norm_gain, in_w)
    part_a, send_b = lax.optimization_barrier((part_a, send_b))
    share_a = row_shares(part_a)
    rows_b = to_group(send_b, expert_count)
    share_b = row_shares(activation_sums(rows_b, norm_gain, in_w))
    share_b, own_keys = lax.optimization_barrier((share_b, own_keys))
    all_keys = lax.all_gather(own_keys, "ctx", axis=1, tiled=True)
    lat_piece, rope_piece = jnp.split(all_keys, [latent_keys.shape[0]], axis=0)
    attn_out = attention(q_latent, q_rope, lat_piece, rope_piece, w_uv)
    hidden_a = activations(share_a, model_width)
    out_a = jnp.dot(hidden_a, down_w, preferred_element_type=jnp.float32).astype(jnp.bfloat16)
    back_a = to_group(out_a, expert_count)
    hidden_b = activations(share_b, model_width)
    out_b = jnp.dot(hidden_b, down_w, preferred_element_type=jnp.float32).astype(jnp.bfloat16)
    back_b = to_group(out_b, expert_count)
    mixed = jnp.dot(weights_a, back_a, preferred_element_type=jnp.float32)
    moe_out = mixed + jnp.dot(weights_b, back_b, preferred_element_type=jnp.float32)
    moe_out = moe_out.astype(jnp.bfloat16)
    return (attn_out, moe_out)


def solution(mesh):
    return jax.shard_map(
        body,
        mesh=mesh,
        in_specs=(
            P(("group", "ctx"), "ep"),
            P(("group", "ctx"), "ep"),
            P("group", "ctx"),
            P("group", "ctx"),
            P("ep", None, None),
            P(("group", "ep"), "ctx"),
            P("ctx"),
            P(("group", "ep"), None),
            P(("group", "ep"), None),
            P("ep", "ctx", None),
            P("ep", "ctx", None),
            P("ep", None, "ctx"),
        ),
        out_specs=(P(("group", "ctx"), "ep"), P(("group", "ep"), "ctx")),
        check_vma=False,
    )
```
